512 devices in a mesh: row: 16 (over x, z_hi, core), col: 32 (over z_lo, y).
Axes of the slice: x: 4, y: 8, z: 8 (z_hi: 2, z_lo: 4; z = z_hi * 4 + z_lo), core: 2. Of those that a mesh axis runs over, the one named last changes fastest.
Arguments:
- points: bfloat16 [12, 16, 512, 64], P(None, 'row', 'col'), may hold values from -7.5 to 7.5
- inverse_factor: bfloat16 [512, 512], replicated, as said below
- panel_index: int32 [1], replicated, may hold values from 15 to 95
- column_map: int32 [32], P('col'), may hold values from 0 to 31, each once
Outputs:
- panel: bfloat16 [6, 16, 512, 512], P(None, 'row', 'col')
- update: bfloat16 [6, 16, 512, 32, 512], P(None, 'row', None, 'col')
The draws below stay inside these ranges and needn't reach their ends.
Inputs may be any that keep to these rules, and one draw needn't show every extreme that they name: `column_map`: a permutation of 0 .. 32 - 1. `inverse_factor`: zero above the diagonal.
All inputs are finite; a program needn't handle non-finite values.
Results may differ from the reference program's by a relative error of at most 0.0049.
Values may be sent and summed in bfloat16 or wider, within the bound.
A program may use at most 64 MiB of HBM per device.

```python
import math
import jax
import jax.numpy as jnp
from jax import lax

NB = 512
DIM = 64
RT = 12
RW = 6
N_ROW = 16
N_COL = 32


def draw_inverse_factor(key, part):
    key_lower, key_diag = jax.random.split(jax.random.fold_in(key, 17))
    indices = jnp.arange(NB)
    below = indices[:, None] > indices[None, :]
    lower_part = jax.random.normal(key_lower, (NB, NB), jnp.float32) * (2.0 / math.sqrt(NB))
    diagonal_part = jax.random.uniform(key_diag, (NB,), jnp.float32, 1.5, 4.5)
    return (jnp.where(below, lower_part, 0.0) + jnp.diag(diagonal_part)).astype(jnp.bfloat16)


def steps_of(own_key, dims, cuts, low, top_value):
    level = 1.0
    for position, parts in cuts:
        draws = jax.random.uniform(jax.random.fold_in(jax.random.fold_in(own_key, 6), position), (parts,), jnp.float32, low / len(cuts), top_value / len(cuts))
        level = level * jnp.repeat(jnp.exp(draws), dims[position] // parts).reshape((-1,) + (1,) * (len(dims) - 1 - position))
    return level


def centred(stream_key, shape, deviation, reach, cuts=(), held_as=jnp.bfloat16):
    factor_of = steps_of(stream_key, shape, cuts, -0.22, 0.18) if cuts else 1.0
    drawn = jax.random.normal(stream_key, shape, jnp.float32) * deviation * factor_of
    return jnp.minimum(jnp.maximum(drawn, -reach), reach).astype(held_as)


def setup_inputs(seed: int = 0) -> dict:
    key_list = jax.random.split(jax.random.key(seed), 5)
    points = centred(key_list[0], (RT, N_ROW, NB, DIM), 2.5, 7.5, ((1, 16), (2, 32)))
    inverse_factor = draw_inverse_factor(jax.random.fold_in(key_list[4], 71), 0)
    panel_index = jax.random.randint(key_list[2], (1,), N_ROW - 1, RT * N_ROW - max(RW * N_ROW, N_COL)).astype(jnp.int32)
    column_map = jax.random.permutation(key_list[3], N_COL).astype(jnp.int32)
    return dict(points=points, inverse_factor=inverse_factor, panel_index=panel_index, column_map=column_map)


JITTER = 1.0


def kern(left_points, right_points):
    left_vals = left_points.astype(jnp.float32)
    right_vals = right_points.astype(jnp.float32)
    inner_products = jnp.einsum('kmd,nd->kmn', left_vals, right_vals, precision=lax.Precision.HIGHEST)
    left_norms = jnp.sum(left_vals * left_vals, axis=-1)
    right_norms = jnp.sum(right_vals * right_vals, axis=-1)
    distance = left_norms[:, :, None] + right_norms[None, None, :] - 2.0 * inner_products
    return jnp.exp(-distance / (2.0 * DIM))


def reference(points, inverse_factor, panel_index, column_map):
    tile_count = RT * N_ROW
    blocks = points.reshape(tile_count, NB, DIM)
    pivot_tile = panel_index[0]
    device_rows = jnp.arange(N_ROW, dtype=jnp.int32)
    start_slot = (pivot_tile + N_ROW - device_rows) // N_ROW
    window_tiles = (start_slot[None, :] + jnp.arange(RW, dtype=jnp.int32)[:, None]) * N_ROW + device_rows[None, :]
    flat_tiles = window_tiles.reshape(RW * N_ROW)
    window_points = blocks[flat_tiles]
    panel_points = blocks[pivot_tile]
    factor_vals = inverse_factor.astype(jnp.float32)

    def panel_of(some_points):
        rounded = kern(some_points, panel_points).astype(jnp.bfloat16)
        rounded = lax.optimization_barrier(rounded).astype(jnp.float32)
        return jnp.einsum('kmn,qn->kmq', rounded, factor_vals).astype(jnp.bfloat16)

    panel_flat = panel_of(window_points)
    panel_tiles = panel_flat.reshape(RW, N_ROW, NB, NB)
    column_tiles = pivot_tile + 1 + column_map
    column_points = blocks[column_tiles]
    column_rows = panel_of(column_points)
    identity = jnp.eye(NB, dtype=jnp.float32)
    panel_vals = panel_flat.astype(jnp.float32)

    def one_column(column_args):
        these_points, these_rows, this_tile = column_args
        update_tile = kern(window_points, these_points)
        update_tile = update_tile + jnp.where(flat_tiles == this_tile, JITTER, 0.0)[:, None, None] * identity
        update_tile = update_tile - jnp.einsum('kmq,nq->kmn', panel_vals, these_rows.astype(jnp.float32))
        return update_tile.astype(jnp.bfloat16)

    updates = lax.map(one_column, (column_points, column_rows, column_tiles))
    updates = updates.reshape(N_COL, RW, N_ROW, NB, NB).transpose(1, 2, 3, 0, 4)
    return panel_tiles, updates
```

```python
import math

import jax
import jax.numpy as jnp
from jax import lax
from jax.experimental import pallas as pl
from jax.experimental.pallas import tpu as pltpu
from jax.sharding import PartitionSpec as P

RW = 6
JITTER = 1.0
NB = 512
DIM = 64
N_ROW = 16
NX, NZH, NCORE, NZL, NY = 4, 2, 2, 4, 8
NZ = NZH * NZL
NP = NX * NCORE
SCALE = math.log2(math.e) / DIM
MESH = pl.DeviceIdType.MESH
BF = jnp.bfloat16
F32 = jnp.float32


def first_slot(p, r):
    return (p + N_ROW - r) // N_ROW


def gather_kernel(
    p_ref, cm_ref, pts_ref, wb, zb,
    xe, xb, ps, yc, yp, cms, zs,
    x_s, x_r, c_s, c_r, wy_s, wy_r, wz_s, wz_r, w2y_s, w2y_r, w2z_s, w2z_r,
    yc_s, yc_r, yp_s, yp_r, z_s, z_r, sw_s, sw_r,
):
    row, col = lax.axis_index("row"), lax.axis_index("col")
    x, zh, core = row // 4, (row // 2) % 2, row % 2
    zl, y = col // NY, col % NY
    z = zh * NZL + zl
    q = x * 2 + core
    p = p_ref[0]

    def dev(x_=x, zh_=zh, core_=core, zl_=zl, y_=y):
        return ((x_ * 2 + zh_) * 2 + core_, zl_ * NY + y_)

    def q_dev(q_):
        return dev(x_=q_ // 2, core_=q_ % 2)

    def z_dev(z_):
        return dev(zh_=z_ // NZL, zl_=z_ % NZL)

    q_peers = [(q + d) % NP for d in range(1, NP)]
    y_peers = [(y + d) % NY for d in range(1, NY)]
    z_peers = [(z + d) % NZ for d in range(1, NZ)]
    l_peers = [(zl + d) % NZL for d in range(1, NZL)]

    barrier = pltpu.get_barrier_semaphore()
    for q_ in q_peers:
        pl.semaphore_signal(barrier, 1, device_id=q_dev(q_), device_id_type=MESH)
    for y_ in y_peers:
        pl.semaphore_signal(barrier, 1, device_id=dev(y_=y_), device_id_type=MESH)
    for z_ in z_peers:
        pl.semaphore_signal(barrier, 1, device_id=z_dev(z_), device_id_type=MESH)

    base = jnp.clip(first_slot(p, row) - 1, 0, pts_ref.shape[0] - RW - 1)
    for t in range(3):
        wb[t, zl, y] = jnp.concatenate([pts_ref[base + 1 + t, 0], pts_ref[base + 4 + t, 0]], axis=1)
    first = pts_ref[base + 1, 0].astype(F32)
    second = pts_ref[base + 2, 0].astype(F32)
    pivot = pts_ref[base, 0].astype(F32)
    cand = jnp.concatenate([first, second], axis=1)
    piv = jnp.concatenate([jnp.zeros_like(pivot), pivot], axis=1)
    for h in range(2):
        rows = slice(8 * h, 8 * h + 8)
        xe[h, 0] = cand[rows].astype(BF)
        xe[h, 1] = piv[rows].astype(BF)
    xb[q] = xe[core]
    cms[zl] = jnp.full((8, 128), cm_ref[0], jnp.int32).astype(F32)
    pl.semaphore_wait(barrier, len(q_peers) + len(y_peers) + len(z_peers))

    sends = []

    def send(src, dst, ssem, rsem, to):
        copy = pltpu.make_async_remote_copy(
            src_ref=src, dst_ref=dst, send_sem=ssem, recv_sem=rsem, device_id=to, device_id_type=MESH
        )
        copy.start()
        sends.append(copy)

    def arrived(dst, rsem):
        pltpu.make_async_remote_copy(
            src_ref=dst, dst_ref=dst, send_sem=rsem, recv_sem=rsem, device_id=dev(), device_id_type=MESH
        ).wait_recv()

    for q_ in q_peers:
        send(xe.at[q_ % 2], xb.at[q], x_s.at[q_], x_r.at[q], q_dev(q_))
    for l_ in l_peers:
        send(cms.at[zl], cms.at[zl], c_s.at[l_], c_r.at[zl], dev(zl_=l_))
    for y_ in y_peers:
        send(wb.at[pl.ds(0, 2), zl, y], wb.at[pl.ds(0, 2), zl, y], wy_s.at[y_], wy_r.at[y], dev(y_=y_))
    for l_ in l_peers:
        send(wb.at[2, zl, y], wb.at[2, zl, y], wz_s.at[l_], wz_r.at[zl], dev(zl_=l_))

    for q_ in q_peers:
        arrived(xb.at[q_], x_r.at[q_])
    mine = jnp.zeros((8, 128), F32)
    for k in range(NP):
        r = ((k // 2) * 2 + zh) * 2 + k % 2
        mine += jnp.where(r == p % N_ROW, xb[k, 1].astype(F32), 0.0)
    ps[...] = mine.astype(BF)
    for y_ in y_peers:
        send(xb.at[:, 0], yc.at[y], yc_s.at[y_], yc_r.at[y], dev(y_=y_))
    yp[y] = mine.astype(BF)
    yc[y] = xb[:, 0]
    for y_ in y_peers:
        send(ps, yp.at[y], yp_s.at[y_], yp_r.at[y], dev(y_=y_))

    for l_ in l_peers:
        arrived(wb.at[2, l_, y], wz_r.at[l_])
    for y_ in y_peers:
        send(wb.at[2, :, y], wb.at[2, :, y], w2y_s.at[y_], w2y_r.at[y], dev(y_=y_))
    for y_ in y_peers:
        arrived(wb.at[pl.ds(0, 2), zl, y_], wy_r.at[y_])
    for l_ in l_peers:
        send(wb.at[pl.ds(0, 2), zl], wb.at[pl.ds(0, 2), zl], w2z_s.at[l_], w2z_r.at[zl], dev(zl_=l_))

    for l_ in l_peers:
        arrived(cms.at[l_], c_r.at[l_])
    for y_ in y_peers:
        arrived(yc.at[y_], yc_r.at[y_])
        arrived(yp.at[y_], yp_r.at[y_])
    lower = lax.broadcasted_iota(jnp.int32, (8, 128), 1) < DIM
    wanted = [cms[l_] for l_ in range(NZL)]
    ranks = []
    for k in range(NP):
        r = ((k // 2) * 2 + zh) * 2 + k % 2
        own = first_slot(p, r) * N_ROW + r - p - 1
        both = jnp.where(lower, own, own + N_ROW).astype(F32)
        ranks.append(both)
    for y_ in range(NY):
        tiles = [yc[y_, k].astype(F32) for k in range(NP)]
        pivot_tile = yp[y_].astype(F32)
        for l_ in range(NZL):
            total = jnp.zeros((8, 128), F32)
            for k in range(NP):
                total = jnp.where(wanted[l_] == ranks[k], tiles[k], total)
            folded = total + pltpu.roll(total, DIM, 1)
            zs[l_, y_] = jnp.where(lower, folded, pivot_tile).astype(BF)
    for z_ in z_peers:
        send(zs.at[z_ % NZL], zb.at[core, z], z_s.at[z_], z_r.at[z], z_dev(z_))
    zb[core, z] = zs[zl]
    other = 1 - core
    for z_ in z_peers:
        arrived(zb.at[core, z_], z_r.at[z_])
        send(zb.at[core, z_], zb.at[core, z_], sw_s.at[z_], sw_r.at[z_], dev(core_=other))
    send(zb.at[core, z], zb.at[core, z], sw_s.at[z], sw_r.at[z], dev(core_=other))

    for l_ in l_peers:
        arrived(wb.at[pl.ds(0, 2), l_], w2z_r.at[l_])
    for y_ in y_peers:
        arrived(wb.at[2, :, y_], w2y_r.at[y_])
    for z_ in range(NZ):
        arrived(zb.at[other, z_], sw_r.at[z_])
    for copy in sends:
        copy.wait_send()


def gathered(panel_index, column_map, points):
    vmem = pl.BlockSpec(memory_space=pltpu.VMEM)
    smem = pl.BlockSpec(memory_space=pltpu.SMEM)
    dma = pltpu.SemaphoreType.DMA
    counts = [NP, NP, NZL, NZL, NY, NY, NZL, NZL, NY, NY, NZL, NZL, NY, NY, NY, NY, NZ, NZ, NZ, NZ]
    return pl.pallas_call(
        gather_kernel,
        out_shape=[
            jax.ShapeDtypeStruct((3, NZL, NY, 16, 128), BF),
            jax.ShapeDtypeStruct((2, NZ, NY, 8, 128), BF),
        ],
        in_specs=[smem, smem, vmem],
        out_specs=[vmem, vmem],
        scratch_shapes=[
            pltpu.VMEM((2, 2, 8, 128), BF),
            pltpu.VMEM((NP, 2, 8, 128), BF),
            pltpu.VMEM((8, 128), BF),
            pltpu.VMEM((NY, NP, 8, 128), BF),
            pltpu.VMEM((NY, 8, 128), BF),
            pltpu.VMEM((NZL, 8, 128), F32),
            pltpu.VMEM((NZL, NY, 8, 128), BF),
        ]
        + [dma((n,)) for n in counts],
        compiler_params=pltpu.CompilerParams(collective_id=0, has_side_effects=True),
        name="gather_points",
    )(panel_index, column_map, points)


def dot(a, b):
    return lax.dot_general(a, b, (((1,), (0,)), ((), ())), preferred_element_type=F32)


def dot_t(a, b):
    return lax.dot_general(a, b, (((1,), (1,)), ((), ())), preferred_element_type=F32)


def tiles_kernel(p_ref, cm_ref, wb, zb, inv, panel_out, update_out, rhs, bias, lcol, panel):
    slot = pl.program_id(0)
    row, col = lax.axis_index("row"), lax.axis_index("col")
    p = p_ref[0]
    half_rows = NB // 2

    @pl.when(slot == 0)
    def _():
        parts = []
        for h in range(2):
            parts.append(zb[h, 0:NZL].astype(F32) + zb[h, NZL:NZ].astype(F32))
        both = jnp.stack(parts, axis=2).reshape(NB, 128)
        flipped = both.T
        squares = flipped * flipped
        for k in range(2):
            one = flipped[k * DIM : (k + 1) * DIM].astype(BF)
            none = jnp.zeros_like(one)
            rhs[0, k] = jnp.concatenate([one, none], axis=0)
            rhs[1, k] = jnp.concatenate([none, one], axis=0)
            bias[k] = jnp.broadcast_to(
                jnp.sum(squares[k * DIM : (k + 1) * DIM], axis=0, keepdims=True) * (0.5 * SCALE), (8, NB)
            )
        lanes = lax.broadcasted_iota(jnp.int32, (NB, 128), 1)
        pivots = both.astype(BF)
        norm = jnp.sum(jnp.where(lanes >= DIM, both * both, 0.0), axis=1, keepdims=True) * (0.5 * SCALE)
        cross = jnp.exp2(SCALE * dot(pivots, rhs[1, 0]) - norm - bias[0, 0:1])
        cross = cross.astype(BF)
        lcol[0:half_rows] = dot(inv[0:half_rows, 0:half_rows], cross[0:half_rows]).astype(BF)
        lcol[half_rows:NB] = dot(inv[half_rows:NB], cross).astype(BF)

    which, half = slot % 3, slot // 3
    tile_row = (first_slot(p, row) + slot) * N_ROW + row
    jitter = jnp.where(tile_row == p + 1 + cm_ref[0], JITTER, 0.0)
    eye = lax.broadcasted_iota(jnp.int32, (128, 128), 0) == lax.broadcasted_iota(jnp.int32, (128, 128), 1)
    diagonal = jnp.where(eye, jitter, 0.0)
    low_lane = half * DIM
    for m in range(2):
        rows = slice(m * half_rows, (m + 1) * half_rows)
        here = wb[which, rows]
        vals = here.astype(F32)
        lanes = lax.broadcasted_iota(jnp.int32, (half_rows, 128), 1)
        inside = (lanes >= low_lane) & (lanes < low_lane + DIM)
        norm = jnp.sum(jnp.where(inside, vals * vals, 0.0), axis=1, keepdims=True) * (0.5 * SCALE)
        kpanel = jnp.exp2(SCALE * dot(here, rhs[half, 1]) - norm - bias[1, 0:1]).astype(BF)
        panel[rows, 0:half_rows] = dot_t(kpanel[:, 0:half_rows], inv[0:half_rows, 0:half_rows]).astype(BF)
        panel[rows, half_rows:NB] = dot_t(kpanel, inv[half_rows:NB]).astype(BF)
        tile = jnp.exp2(SCALE * dot(here, rhs[half, 0]) - norm - bias[0, 0:1])
        product = dot(panel[rows], lcol[...])
        for i in range(2):
            sub = slice(i * 128, (i + 1) * 128)
            out_rows = slice(m * half_rows + i * 128, m * half_rows + (i + 1) * 128)
            for j in range(4):
                cols = slice(j * 128, (j + 1) * 128)
                value = tile[sub, cols]
                if j == 2 * m + i:
                    value = value + diagonal
                update_out[0, out_rows, cols] = (value - product[sub, cols]).astype(BF)
    start = pl.multiple_of(col * 16, 16)
    panel_out[slot] = panel[pl.ds(start, 16)]


def tiles(panel_index, column_map, wb, zb, inverse_factor):
    smem = pl.BlockSpec(memory_space=pltpu.SMEM)

    def whole(shape):
        return pl.BlockSpec(shape, lambda i: (0,) * len(shape))

    flops = 2 * NB * NB * (RW * (2 * 128 + 2 * NB) + 2 * NB)
    return pl.pallas_call(
        tiles_kernel,
        grid=(RW,),
        out_shape=[
            jax.ShapeDtypeStruct((RW, 16, NB), BF),
            jax.ShapeDtypeStruct((RW, NB, NB), BF),
        ],
        in_specs=[smem, smem, whole((3, NB, 128)), whole((2, NZ, NY, 8, 128)), whole((NB, NB))],
        out_specs=[whole((RW, 16, NB)), pl.BlockSpec((1, NB, NB), lambda i: (i, 0, 0))],
        scratch_shapes=[
            pltpu.VMEM((2, 2, 128, NB), BF),
            pltpu.VMEM((2, 8, NB), F32),
            pltpu.VMEM((NB, NB), BF),
            pltpu.VMEM((NB, NB), BF),
        ],
        cost_estimate=pl.CostEstimate(flops=flops, bytes_accessed=5 << 20, transcendentals=13 * NB * NB),
        name="window_tiles",
    )(panel_index, column_map, wb, zb, inverse_factor)


def shards(points, inverse_factor, panel_index, column_map):
    wb, zb = gathered(panel_index, column_map, points)
    panel_part, update = tiles(panel_index, column_map, wb.reshape(3, NB, 128), zb, inverse_factor)
    return panel_part[:, None], update[:, None, :, None, :]


def solution(mesh):
    in_specs = (P(None, "row", "col", None), P(), P(), P("col"))
    out_specs = (P(None, "row", "col", None), P(None, "row", None, "col", None))
    return jax.shard_map(shards, mesh=mesh, in_specs=in_specs, out_specs=out_specs, check_vma=False)
```

```python
import math

import jax
import jax.numpy as jnp
from jax import lax
from jax.experimental import pallas as pl
from jax.experimental.pallas import tpu as pltpu
from jax.sharding import PartitionSpec as P

RW = 6
JITTER = 1.0
NB = 512
DIM = 64
N_ROW = 16
NX, NZH, NCORE, NZL, NY = 4, 2, 2, 4, 8
NZ = NZH * NZL
NP = NX * NCORE
SCALE = math.log2(math.e) / DIM
MESH = pl.DeviceIdType.MESH
BF = jnp.bfloat16
F32 = jnp.float32


def first_slot(p, r):
    return (p + N_ROW - r) // N_ROW


def assembled(buf):
    low = lax.broadcasted_iota(jnp.int32, (8, 128), 1) < DIM
    parts = []
    for h in range(2):
        packed = buf[h, 0:NZL].astype(F32) + buf[h, NZL:NZ].astype(F32)
        turned = pltpu.roll(packed.reshape(NZL * 4 * 8, 128), DIM, 1).reshape(packed.shape)
        parts.append(jnp.where(low, jnp.concatenate([packed, turned], axis=1), 0.0))
    return jnp.stack(parts, axis=2).reshape(NB, 128)


def packed_pair(a, b, low):
    return jnp.where(low, a, pltpu.roll(b, DIM, 1))


def fill_rhs(block, rhs, bias):
    turned = block.T[0:DIM]
    one = turned.astype(BF)
    none = jnp.zeros_like(one)
    rhs[0] = jnp.concatenate([one, none], axis=0)
    rhs[1] = jnp.concatenate([none, one], axis=0)
    norm = jnp.sum(turned * turned, axis=0, keepdims=True) * (0.5 * SCALE)
    bias[...] = jnp.broadcast_to(norm, (8, NB))


def row_norm(vals, low_lane):
    lanes = lax.broadcasted_iota(jnp.int32, vals.shape, 1)
    inside = (lanes >= low_lane) & (lanes < low_lane + DIM)
    return jnp.sum(jnp.where(inside, vals * vals, 0.0), axis=1, keepdims=True) * (0.5 * SCALE)


def dot(a, b):
    return lax.dot_general(a, b, (((1,), (0,)), ((), ())), preferred_element_type=F32)


def dot_t(a, b):
    return lax.dot_general(a, b, (((1,), (1,)), ((), ())), preferred_element_type=F32)


def gather_kernel(
    p_hbm, cm_hbm, pts_hbm, inv_hbm, wb, zc, xp, panel, inv,
    p_ref, cm_ref, pts_ref, xe, xb, ps, yc, yp, cms, zs, zq, zp, rhs, bias,
    x_s, x_r, c_s, c_r, wy_s, wy_r, wz_s, wz_r, w2y_s, w2y_r, w2z_s, w2z_r,
    yc_s, yc_r, yp_s, yp_r, zp_s, zp_r, zc_s, zc_r, in_s,
):
    row, col = lax.axis_index("row"), lax.axis_index("col")
    x, zh, core = row // 4, (row // 2) % 2, row % 2
    zl, y = col // NY, col % NY
    z = zh * NZL + zl
    q = x * 2 + core

    def dev(x_=x, zh_=zh, core_=core, zl_=zl, y_=y):
        return ((x_ * 2 + zh_) * 2 + core_, zl_ * NY + y_)

    def q_dev(q_):
        return dev(x_=q_ // 2, core_=q_ % 2)

    def z_dev(z_, core_):
        return dev(zh_=z_ // NZL, zl_=z_ % NZL, core_=core_)

    q_peers = [(q + d) % NP for d in range(1, NP)]
    y_peers = [(y + d) % NY for d in range(1, NY)]
    z_peers = [(z + d) % NZ for d in range(1, NZ)]
    l_peers = [(zl + d) % NZL for d in range(1, NZL)]
    line = [(z_, (core + k) % 2) for z_ in z_peers for k in range(2)] + [(z, 1 - core)]

    barrier = pltpu.get_barrier_semaphore()
    for q_ in q_peers:
        pl.semaphore_signal(barrier, 1, device_id=q_dev(q_), device_id_type=MESH)
    for y_ in y_peers:
        pl.semaphore_signal(barrier, 1, device_id=dev(y_=y_), device_id_type=MESH)
    for z_, k_ in line[:-1]:
        pl.semaphore_signal(barrier, 1, device_id=z_dev(z_, k_), device_id_type=MESH)

    loads = [
        pltpu.make_async_copy(src, dst, in_s.at[i])
        for i, (src, dst) in enumerate(
            [(p_hbm, p_ref), (cm_hbm, cm_ref), (pts_hbm, pts_ref), (inv_hbm, inv)]
        )
    ]
    for load in loads:
        load.start()
    for load in loads[:3]:
        load.wait()
    p = p_ref[0]

    base = jnp.clip(first_slot(p, row) - 1, 0, pts_ref.shape[0] - RW - 1)
    for t in range(3):
        wb[t, zl, y] = jnp.concatenate([pts_ref[base + 1 + t, 0], pts_ref[base + 4 + t, 0]], axis=1)
    first = pts_ref[base + 1, 0].astype(F32)
    second = pts_ref[base + 2, 0].astype(F32)
    pivot = pts_ref[base, 0].astype(F32)
    cand = jnp.concatenate([first, second], axis=1)
    piv = jnp.concatenate([pivot, jnp.zeros_like(pivot)], axis=1)
    for h in range(2):
        rows = slice(8 * h, 8 * h + 8)
        xe[h, 0] = cand[rows].astype(BF)
        xe[h, 1] = piv[rows].astype(BF)
    xb[q] = xe[core]
    cms[zl] = jnp.full((8, 128), cm_ref[0], jnp.int32).astype(F32)
    pl.semaphore_wait(barrier, len(q_peers) + len(y_peers) + len(line) - 1)

    sends = []

    def send(src, dst, ssem, rsem, to):
        copy = pltpu.make_async_remote_copy(
            src_ref=src, dst_ref=dst, send_sem=ssem, recv_sem=rsem, device_id=to, device_id_type=MESH
        )
        copy.start()
        sends.append(copy)

    def arrived(dst, rsem):
        pltpu.make_async_remote_copy(
            src_ref=dst, dst_ref=dst, send_sem=rsem, recv_sem=rsem, device_id=dev(), device_id_type=MESH
        ).wait_recv()

    def send_line(src_of, dst, ssem, rsem):
        for z_, k_ in line:
            send(src_of(z_), dst.at[core, z], ssem.at[k_ * NZ + z_], rsem.at[core * NZ + z], z_dev(z_, k_))

    def line_arrived(dst, rsem):
        for z_, k_ in line:
            arrived(dst.at[k_, z_], rsem.at[k_ * NZ + z_])

    zfirst, yfirst = pl.ds(0, 2), pl.ds(2, 1)
    for q_ in q_peers:
        send(xe.at[q_ % 2], xb.at[q], x_s.at[q_], x_r.at[q], q_dev(q_))
    for l_ in l_peers:
        send(cms.at[zl], cms.at[zl], c_s.at[l_], c_r.at[zl], dev(zl_=l_))
    for y_ in y_peers:
        send(wb.at[yfirst, zl, y], wb.at[yfirst, zl, y], wy_s.at[y_], wy_r.at[y], dev(y_=y_))
    for l_ in l_peers:
        send(wb.at[zfirst, zl, y], wb.at[zfirst, zl, y], wz_s.at[l_], wz_r.at[zl], dev(zl_=l_))

    for q_ in q_peers:
        arrived(xb.at[q_], x_r.at[q_])
    mine = jnp.zeros((8, 128), F32)
    for k in range(NP):
        r = ((k // 2) * 2 + zh) * 2 + k % 2
        mine += jnp.where(r == p % N_ROW, xb[k, 1].astype(F32), 0.0)
    ps[...] = mine.astype(BF)
    yp[y] = mine.astype(BF)
    yc[y] = xb[:, 0]
    for y_ in y_peers:
        send(ps, yp.at[y], yp_s.at[y_], yp_r.at[y], dev(y_=y_))
    for y_ in y_peers:
        send(xb.at[:, 0], yc.at[y], yc_s.at[y_], yc_r.at[y], dev(y_=y_))

    for l_ in l_peers:
        arrived(wb.at[zfirst, l_, y], wz_r.at[l_])
    for y_ in y_peers:
        send(wb.at[zfirst, :, y], wb.at[zfirst, :, y], w2y_s.at[y_], w2y_r.at[y], dev(y_=y_))
    for y_ in y_peers:
        arrived(wb.at[yfirst, zl, y_], wy_r.at[y_])
    for l_ in l_peers:
        send(wb.at[yfirst, zl], wb.at[yfirst, zl], w2z_s.at[l_], w2z_r.at[zl], dev(zl_=l_))

    low = lax.broadcasted_iota(jnp.int32, (8, 128), 1) < DIM
    for y_ in y_peers:
        arrived(yp.at[y_], yp_r.at[y_])
    for k in range(4):
        zq[k] = packed_pair(yp[k].astype(F32), yp[k + 4].astype(F32), low).astype(BF)
    zp[core, z] = zq[...]
    send_line(lambda z_: zq, zp, zp_s, zp_r)

    for l_ in l_peers:
        arrived(cms.at[l_], c_r.at[l_])
    wanted = [cms[l_] for l_ in range(NZL)]
    ranks = []
    for k in range(NP):
        r = ((k // 2) * 2 + zh) * 2 + k % 2
        own = first_slot(p, r) * N_ROW + r - p - 1
        ranks.append(jnp.where(low, own, own + N_ROW).astype(F32))
    for y_ in y_peers:
        arrived(yc.at[y_], yc_r.at[y_])
    for k4 in range(4):
        chosen = [[], []]
        for i in range(2):
            tiles = [yc[k4 + 4 * i, k].astype(F32) for k in range(NP)]
            for l_ in range(NZL):
                total = jnp.zeros((8, 128), F32)
                for k in range(NP):
                    total = jnp.where(wanted[l_] == ranks[k], tiles[k], total)
                chosen[i].append(total + pltpu.roll(total, DIM, 1))
        for l_ in range(NZL):
            zs[l_, k4] = jnp.where(low, chosen[0][l_], chosen[1][l_]).astype(BF)
    zc[core, z] = zs[zl]
    send_line(lambda z_: zs.at[z_ % NZL], zc, zc_s, zc_r)

    line_arrived(zp, zp_r)
    pivots = assembled(zp)
    xp[...] = pivots.astype(BF)
    fill_rhs(pivots, rhs, bias)
    for l_ in l_peers:
        arrived(wb.at[yfirst, l_], w2z_r.at[l_])
    for y_ in y_peers:
        arrived(wb.at[zfirst, :, y_], w2y_r.at[y_])

    loads[3].wait()
    half_rows = NB // 2

    @pl.loop(0, RW)
    def _(slot):
        which, half = slot % 3, slot // 3
        for m in range(2):
            rows = slice(m * half_rows, (m + 1) * half_rows)
            here = wb[which, 2 * m : 2 * m + 2].reshape(half_rows, 128)
            norm = row_norm(here.astype(F32), half * DIM)
            kpanel = jnp.exp2(SCALE * dot(here, rhs[half]) - norm - bias[0:1]).astype(BF)
            panel[slot, rows, 0:half_rows] = dot_t(
                kpanel[:, 0:half_rows], inv[0:half_rows, 0:half_rows]
            ).astype(BF)
            panel[slot, rows, half_rows:NB] = dot_t(kpanel, inv[half_rows:NB]).astype(BF)

    line_arrived(zc, zc_r)
    for copy in sends:
        copy.wait_send()


def gathered(panel_index, column_map, points, inverse_factor):
    vmem = pl.BlockSpec(memory_space=pltpu.VMEM)
    hbm = pl.BlockSpec(memory_space=pltpu.HBM)
    dma = pltpu.SemaphoreType.DMA
    counts = [NP, NP, NZL, NZL, NY, NY, NZL, NZL, NY, NY, NZL, NZL, NY, NY, NY, NY] + [2 * NZ] * 4 + [4]
    return pl.pallas_call(
        gather_kernel,
        out_shape=[
            pltpu.VMEM((3, NZL, NY, 16, 128), BF),
            pltpu.VMEM((2, NZ, 4, 8, 128), BF),
            pltpu.VMEM((NB, 128), BF),
            pltpu.VMEM((RW, NB, NB), BF),
            pltpu.VMEM((NB, NB), BF),
        ],
        in_specs=[hbm] * 4,
        out_specs=[vmem] * 5,
        scratch_shapes=[
            pltpu.SMEM((1,), jnp.int32),
            pltpu.SMEM((1,), jnp.int32),
            pltpu.VMEM(points.shape, BF),
            pltpu.VMEM((2, 2, 8, 128), BF),
            pltpu.VMEM((NP, 2, 8, 128), BF),
            pltpu.VMEM((8, 128), BF),
            pltpu.VMEM((NY, NP, 8, 128), BF),
            pltpu.VMEM((NY, 8, 128), BF),
            pltpu.VMEM((NZL, 8, 128), F32),
            pltpu.VMEM((NZL, 4, 8, 128), BF),
            pltpu.VMEM((4, 8, 128), BF),
            pltpu.VMEM((2, NZ, 4, 8, 128), BF),
            pltpu.VMEM((2, 128, NB), BF),
            pltpu.VMEM((8, NB), F32),
        ]
        + [dma((n,)) for n in counts],
        compiler_params=pltpu.CompilerParams(collective_id=0, has_side_effects=True, vmem_limit_bytes=61100 << 10),
        name="gather_panel",
    )(panel_index, column_map, points, inverse_factor)


def tiles_kernel(
    p_hbm, cm_hbm, wb, zc, xp, inv, panel, panel_out, update_out, rhs, bias, lcol, p_ref, cm_ref, in_s
):
    slot = pl.program_id(0)
    row, col = lax.axis_index("row"), lax.axis_index("col")
    half_rows = NB // 2

    @pl.when(slot == 0)
    def _():
        loads = [
            pltpu.make_async_copy(p_hbm, p_ref, in_s.at[0]),
            pltpu.make_async_copy(cm_hbm, cm_ref, in_s.at[1]),
        ]
        for load in loads:
            load.start()
        fill_rhs(assembled(zc), rhs, bias)
        norm = row_norm(xp[...].astype(F32), 0)
        cross = jnp.exp2(SCALE * dot(xp[...], rhs[0]) - norm - bias[0:1]).astype(BF)
        lcol[0:half_rows] = dot(inv[0:half_rows, 0:half_rows], cross[0:half_rows]).astype(BF)
        lcol[half_rows:NB] = dot(inv[half_rows:NB], cross).astype(BF)
        start = pl.multiple_of(col * 16, 16)
        for a in range(RW):
            panel_out[a] = panel[a, pl.ds(start, 16)]
        for load in loads:
            load.wait()

    p = p_ref[0]
    which, half = slot % 3, slot // 3
    tile_row = (first_slot(p, row) + slot) * N_ROW + row
    jitter = jnp.where(tile_row == p + 1 + cm_ref[0], JITTER, 0.0)
    eye = lax.broadcasted_iota(jnp.int32, (128, 128), 0) == lax.broadcasted_iota(jnp.int32, (128, 128), 1)
    diagonal = jnp.where(eye, jitter, 0.0)
    for m in range(2):
        rows = slice(m * half_rows, (m + 1) * half_rows)
        here = wb[which, 2 * m : 2 * m + 2].reshape(half_rows, 128)
        norm = row_norm(here.astype(F32), half * DIM)
        tile = jnp.exp2(SCALE * dot(here, rhs[half]) - norm - bias[0:1])
        product = dot(panel[slot, rows], lcol[...])
        for i in range(2):
            sub = slice(i * 128, (i + 1) * 128)
            out_rows = slice(m * half_rows + i * 128, m * half_rows + (i + 1) * 128)
            for j in range(4):
                cols = slice(j * 128, (j + 1) * 128)
                value = tile[sub, cols]
                if j == 2 * m + i:
                    value = value + diagonal
                update_out[0, out_rows, cols] = (value - product[sub, cols]).astype(BF)


def tiles(panel_index, column_map, wb, zc, xp, inverse_factor, panel):
    vmem = pl.BlockSpec(memory_space=pltpu.VMEM)
    hbm = pl.BlockSpec(memory_space=pltpu.HBM)
    flops = 2 * NB * NB * (RW * (128 + NB) + 2 * NB)
    return pl.pallas_call(
        tiles_kernel,
        grid=(RW,),
        out_shape=[
            jax.ShapeDtypeStruct((RW, 16, NB), BF),
            jax.ShapeDtypeStruct((RW, NB, NB), BF),
        ],
        in_specs=[hbm, hbm, vmem, vmem, vmem, vmem, vmem],
        out_specs=[
            pl.BlockSpec((RW, 16, NB), lambda i: (0, 0, 0)),
            pl.BlockSpec((1, NB, NB), lambda i: (i, 0, 0)),
        ],
        scratch_shapes=[
            pltpu.VMEM((2, 128, NB), BF),
            pltpu.VMEM((8, NB), F32),
            pltpu.VMEM((NB, NB), BF),
            pltpu.SMEM((1,), jnp.int32),
            pltpu.SMEM((1,), jnp.int32),
            pltpu.SemaphoreType.DMA((2,)),
        ],
        compiler_params=pltpu.CompilerParams(vmem_limit_bytes=24 << 20),
        cost_estimate=pl.CostEstimate(flops=flops, bytes_accessed=5 << 20, transcendentals=7 * NB * NB),
        name="window_tiles",
    )(panel_index, column_map, wb, zc, xp, inverse_factor, panel)


def shards(points, inverse_factor, panel_index, column_map):
    wb, zc, xp, panel, inv = gathered(panel_index, column_map, points, inverse_factor)
    panel_part, update = tiles(panel_index, column_map, wb, zc, xp, inv, panel)
    return panel_part[:, None], update[:, None, :, None, :]


def solution(mesh):
    in_specs = (P(None, "row", "col", None), P(), P(), P("col"))
    out_specs = (P(None, "row", "col", None), P(None, "row", None, "col", None))
    return jax.shard_map(shards, mesh=mesh, in_specs=in_specs, out_specs=out_specs, check_vma=False)
```

```python
import math

import jax
import jax.numpy as jnp
from jax import lax
from jax.experimental import pallas as pl
from jax.experimental.pallas import tpu as pltpu
from jax.sharding import PartitionSpec as P

RW = 6
JITTER = 1.0
NB = 512
DIM = 64
N_ROW = 16
NX, NZH, NCORE, NZL, NY = 4, 2, 2, 4, 8
NZ = NZH * NZL
NP = NX * NCORE
SCALE = math.log2(math.e) / DIM
MESH = pl.DeviceIdType.MESH
BF = jnp.bfloat16
F32 = jnp.float32


def first_slot(p, r):
    return (p + N_ROW - r) // N_ROW


def assembled(buf):
    low = lax.broadcasted_iota(jnp.int32, (8, 128), 1) < DIM
    parts = []
    for h in range(2):
        packed = buf[h, 0:NZL].astype(F32) + buf[h, NZL:NZ].astype(F32)
        turned = pltpu.roll(packed.reshape(NZL * 4 * 8, 128), DIM, 1).reshape(packed.shape)
        parts.append(jnp.where(low, jnp.concatenate([packed, turned], axis=1), 0.0))
    return jnp.stack(parts, axis=2).reshape(NB, 128)


def packed_pair(a, b, low):
    return jnp.where(low, a, pltpu.roll(b, DIM, 1))


def fill_rhs(block, rhs, bias):
    turned = block.T[0:DIM]
    one = turned.astype(BF)
    none = jnp.zeros_like(one)
    rhs[0] = jnp.concatenate([one, none], axis=0)
    rhs[1] = jnp.concatenate([none, one], axis=0)
    norm = jnp.sum(turned * turned, axis=0, keepdims=True) * (0.5 * SCALE)
    bias[...] = jnp.broadcast_to(norm, (8, NB))


def row_norm(vals, low_lane):
    lanes = lax.broadcasted_iota(jnp.int32, vals.shape, 1)
    inside = (lanes >= low_lane) & (lanes < low_lane + DIM)
    return jnp.sum(jnp.where(inside, vals * vals, 0.0), axis=1, keepdims=True) * (0.5 * SCALE)


def dot(a, b):
    return lax.dot_general(a, b, (((1,), (0,)), ((), ())), preferred_element_type=F32)


def dot_t(a, b):
    return lax.dot_general(a, b, (((1,), (1,)), ((), ())), preferred_element_type=F32)


def gather_kernel(
    p_hbm, cm_hbm, pts_hbm, inv_hbm, wb, zc, xp, panel, inv,
    p_ref, cm_ref, pts_ref, xe, xb, ps, yc, yp, cms, zs, zq, zp, rhs, bias,
    x_s, x_r, c_s, c_r, wy_s, wy_r, wz_s, wz_r, w2y_s, w2y_r, w2z_s, w2z_r,
    yc_s, yc_r, yp_s, yp_r, zp_s, zp_r, zc_s, zc_r, in_s, rounds,
):
    row, col = lax.axis_index("row"), lax.axis_index("col")
    x, zh, core = row // 4, (row // 2) % 2, row % 2
    zl, y = col // NY, col % NY
    z = zh * NZL + zl
    q = x * 2 + core

    def dev(x_=x, zh_=zh, core_=core, zl_=zl, y_=y):
        return ((x_ * 2 + zh_) * 2 + core_, zl_ * NY + y_)

    def q_dev(q_):
        return dev(x_=q_ // 2, core_=q_ % 2)

    def z_dev(z_, core_):
        return dev(zh_=z_ // NZL, zl_=z_ % NZL, core_=core_)

    q_peers = [(q + d) % NP for d in range(1, NP)]
    y_peers = [(y + d) % NY for d in range(1, NY)]
    z_peers = [(z + d) % NZ for d in range(1, NZ)]
    l_peers = [(zl + d) % NZL for d in range(1, NZL)]
    line = [(z_, (core + k) % 2) for z_ in z_peers for k in range(2)] + [(z, 1 - core)]

    loads = [
        pltpu.make_async_copy(src, dst, in_s.at[i])
        for i, (src, dst) in enumerate(
            [(p_hbm, p_ref), (cm_hbm, cm_ref), (pts_hbm, pts_ref), (inv_hbm, inv)]
        )
    ]
    for load in loads:
        load.start()

    barrier = pltpu.get_barrier_semaphore()
    y_near = [(y + 1) % NY, (y + NY - 1) % NY]
    z_near = [(z + 1) % NZ, (z + NZ - 1) % NZ]
    near = [dev(y_=y_) for y_ in y_near] + [z_dev(z_, core) for z_ in z_near]
    greeted = [q_dev(q_) for q_ in q_peers] + near + [z_dev(z_, 1 - core) for z_ in z_near]
    for to in greeted:
        pl.semaphore_signal(barrier, 1, device_id=to, device_id_type=MESH)

    for load in loads[:3]:
        load.wait()
    p = p_ref[0]

    base = jnp.clip(first_slot(p, row) - 1, 0, pts_ref.shape[0] - RW - 1)
    for t in range(3):
        wb[t, zl, y] = jnp.concatenate([pts_ref[base + 1 + t, 0], pts_ref[base + 4 + t, 0]], axis=1)
    first = pts_ref[base + 1, 0].astype(F32)
    second = pts_ref[base + 2, 0].astype(F32)
    pivot = pts_ref[base, 0].astype(F32)
    cand = jnp.concatenate([first, second], axis=1)
    piv = jnp.concatenate([pivot, jnp.zeros_like(pivot)], axis=1)
    for h in range(2):
        rows = slice(8 * h, 8 * h + 8)
        xe[h, 0] = cand[rows].astype(BF)
        xe[h, 1] = piv[rows].astype(BF)
    xb[q] = xe[core]
    cms[zl] = jnp.full((8, 128), cm_ref[0], jnp.int32).astype(F32)
    pl.semaphore_wait(barrier, len(greeted))

    sends = []

    def send(src, dst, ssem, rsem, to):
        copy = pltpu.make_async_remote_copy(
            src_ref=src, dst_ref=dst, send_sem=ssem, recv_sem=rsem, device_id=to, device_id_type=MESH
        )
        copy.start()
        sends.append(copy)

    def arrived(dst, rsem):
        pltpu.make_async_remote_copy(
            src_ref=dst, dst_ref=dst, send_sem=rsem, recv_sem=rsem, device_id=dev(), device_id_type=MESH
        ).wait_recv()

    def send_line(src_of, dst, ssem, rsem):
        for z_, k_ in line:
            send(src_of(z_), dst.at[core, z], ssem.at[k_ * NZ + z_], rsem.at[core * NZ + z], z_dev(z_, k_))

    def line_arrived(dst, rsem):
        for z_, k_ in line:
            arrived(dst.at[k_, z_], rsem.at[k_ * NZ + z_])

    zfirst, yfirst = pl.ds(0, 2), pl.ds(2, 1)
    for q_ in q_peers:
        send(xe.at[q_ % 2], xb.at[q], x_s.at[q_], x_r.at[q], q_dev(q_))
    for k in range(NY // 2 - 1):
        for to in near:
            pl.semaphore_signal(rounds.at[k], 1, device_id=to, device_id_type=MESH)
        pl.semaphore_wait(rounds.at[k], len(near))
    for l_ in l_peers:
        send(cms.at[zl], cms.at[zl], c_s.at[l_], c_r.at[zl], dev(zl_=l_))
    for y_ in y_peers:
        send(wb.at[yfirst, zl, y], wb.at[yfirst, zl, y], wy_s.at[y_], wy_r.at[y], dev(y_=y_))
    for l_ in l_peers:
        send(wb.at[zfirst, zl, y], wb.at[zfirst, zl, y], wz_s.at[l_], wz_r.at[zl], dev(zl_=l_))

    for q_ in q_peers:
        arrived(xb.at[q_], x_r.at[q_])
    mine = jnp.zeros((8, 128), F32)
    for k in range(NP):
        r = ((k // 2) * 2 + zh) * 2 + k % 2
        mine += jnp.where(r == p % N_ROW, xb[k, 1].astype(F32), 0.0)
    ps[...] = mine.astype(BF)
    yp[y] = mine.astype(BF)
    yc[y] = xb[:, 0]
    for y_ in y_peers:
        send(ps, yp.at[y], yp_s.at[y_], yp_r.at[y], dev(y_=y_))
    for y_ in y_peers:
        send(xb.at[:, 0], yc.at[y], yc_s.at[y_], yc_r.at[y], dev(y_=y_))

    for l_ in l_peers:
        arrived(wb.at[zfirst, l_, y], wz_r.at[l_])
    for y_ in y_peers:
        send(wb.at[zfirst, :, y], wb.at[zfirst, :, y], w2y_s.at[y_], w2y_r.at[y], dev(y_=y_))
    for y_ in y_peers:
        arrived(wb.at[yfirst, zl, y_], wy_r.at[y_])
    for l_ in l_peers:
        send(wb.at[yfirst, zl], wb.at[yfirst, zl], w2z_s.at[l_], w2z_r.at[zl], dev(zl_=l_))

    low = lax.broadcasted_iota(jnp.int32, (8, 128), 1) < DIM
    for y_ in y_peers:
        arrived(yp.at[y_], yp_r.at[y_])
    for k in range(4):
        zq[k] = packed_pair(yp[k].astype(F32), yp[k + 4].astype(F32), low).astype(BF)
    zp[core, z] = zq[...]
    send_line(lambda z_: zq, zp, zp_s, zp_r)

    for l_ in l_peers:
        arrived(cms.at[l_], c_r.at[l_])
    wanted = [cms[l_] for l_ in range(NZL)]
    ranks = []
    for k in range(NP):
        r = ((k // 2) * 2 + zh) * 2 + k % 2
        own = first_slot(p, r) * N_ROW + r - p - 1
        ranks.append(jnp.where(low, own, own + N_ROW).astype(F32))
    for y_ in y_peers:
        arrived(yc.at[y_], yc_r.at[y_])
    for k4 in range(4):
        chosen = [[], []]
        for i in range(2):
            tiles = [yc[k4 + 4 * i, k].astype(F32) for k in range(NP)]
            for l_ in range(NZL):
                total = jnp.zeros((8, 128), F32)
                for k in range(NP):
                    total = jnp.where(wanted[l_] == ranks[k], tiles[k], total)
                chosen[i].append(total + pltpu.roll(total, DIM, 1))
        for l_ in range(NZL):
            zs[l_, k4] = jnp.where(low, chosen[0][l_], chosen[1][l_]).astype(BF)
    zc[core, z] = zs[zl]
    send_line(lambda z_: zs.at[z_ % NZL], zc, zc_s, zc_r)

    line_arrived(zp, zp_r)
    pivots = assembled(zp)
    xp[...] = pivots.astype(BF)
    fill_rhs(pivots, rhs, bias)
    for l_ in l_peers:
        arrived(wb.at[yfirst, l_], w2z_r.at[l_])
    for y_ in y_peers:
        arrived(wb.at[zfirst, :, y_], w2y_r.at[y_])

    loads[3].wait()
    half_rows = NB // 2

    @pl.loop(0, RW)
    def _(slot):
        which, half = slot % 3, slot // 3
        for m in range(2):
            rows = slice(m * half_rows, (m + 1) * half_rows)
            here = wb[which, 2 * m : 2 * m + 2].reshape(half_rows, 128)
            norm = row_norm(here.astype(F32), half * DIM)
            kpanel = jnp.exp2(SCALE * dot(here, rhs[half]) - norm - bias[0:1]).astype(BF)
            panel[slot, rows, 0:half_rows] = dot_t(
                kpanel[:, 0:half_rows], inv[0:half_rows, 0:half_rows]
            ).astype(BF)
            panel[slot, rows, half_rows:NB] = dot_t(kpanel, inv[half_rows:NB]).astype(BF)

    line_arrived(zc, zc_r)
    for copy in sends:
        copy.wait_send()


def gathered(panel_index, column_map, points, inverse_factor):
    vmem = pl.BlockSpec(memory_space=pltpu.VMEM)
    hbm = pl.BlockSpec(memory_space=pltpu.HBM)
    dma = pltpu.SemaphoreType.DMA
    counts = [NP, NP, NZL, NZL, NY, NY, NZL, NZL, NY, NY, NZL, NZL, NY, NY, NY, NY] + [2 * NZ] * 4 + [4]
    return pl.pallas_call(
        gather_kernel,
        out_shape=[
            pltpu.VMEM((3, NZL, NY, 16, 128), BF),
            pltpu.VMEM((2, NZ, 4, 8, 128), BF),
            pltpu.VMEM((NB, 128), BF),
            pltpu.VMEM((RW, NB, NB), BF),
            pltpu.VMEM((NB, NB), BF),
        ],
        in_specs=[hbm] * 4,
        out_specs=[vmem] * 5,
        scratch_shapes=[
            pltpu.SMEM((1,), jnp.int32),
            pltpu.SMEM((1,), jnp.int32),
            pltpu.VMEM(points.shape, BF),
            pltpu.VMEM((2, 2, 8, 128), BF),
            pltpu.VMEM((NP, 2, 8, 128), BF),
            pltpu.VMEM((8, 128), BF),
            pltpu.VMEM((NY, NP, 8, 128), BF),
            pltpu.VMEM((NY, 8, 128), BF),
            pltpu.VMEM((NZL, 8, 128), F32),
            pltpu.VMEM((NZL, 4, 8, 128), BF),
            pltpu.VMEM((4, 8, 128), BF),
            pltpu.VMEM((2, NZ, 4, 8, 128), BF),
            pltpu.VMEM((2, 128, NB), BF),
            pltpu.VMEM((8, NB), F32),
        ]
        + [dma((n,)) for n in counts]
        + [pltpu.SemaphoreType.REGULAR((NY // 2 - 1,))],
        compiler_params=pltpu.CompilerParams(collective_id=0, has_side_effects=True, vmem_limit_bytes=61100 << 10),
        name="gather_panel",
    )(panel_index, column_map, points, inverse_factor)


def tiles_kernel(
    p_hbm, cm_hbm, wb, zc, xp, inv, panel, panel_out, update_out, rhs, bias, lcol, p_ref, cm_ref, in_s
):
    slot = pl.program_id(0)
    row, col = lax.axis_index("row"), lax.axis_index("col")
    half_rows = NB // 2

    @pl.when(slot == 0)
    def _():
        loads = [
            pltpu.make_async_copy(p_hbm, p_ref, in_s.at[0]),
            pltpu.make_async_copy(cm_hbm, cm_ref, in_s.at[1]),
        ]
        for load in loads:
            load.start()
        fill_rhs(assembled(zc), rhs, bias)
        norm = row_norm(xp[...].astype(F32), 0)
        cross = jnp.exp2(SCALE * dot(xp[...], rhs[0]) - norm - bias[0:1]).astype(BF)
        lcol[0:half_rows] = dot(inv[0:half_rows, 0:half_rows], cross[0:half_rows]).astype(BF)
        lcol[half_rows:NB] = dot(inv[half_rows:NB], cross).astype(BF)
        start = pl.multiple_of(col * 16, 16)
        for a in range(RW):
            panel_out[a] = panel[a, pl.ds(start, 16)]
        for load in loads:
            load.wait()

    p = p_ref[0]
    which, half = slot % 3, slot // 3
    tile_row = (first_slot(p, row) + slot) * N_ROW + row
    jitter = jnp.where(tile_row == p + 1 + cm_ref[0], JITTER, 0.0)
    eye = lax.broadcasted_iota(jnp.int32, (128, 128), 0) == lax.broadcasted_iota(jnp.int32, (128, 128), 1)
    diagonal = jnp.where(eye, jitter, 0.0)
    for m in range(2):
        rows = slice(m * half_rows, (m + 1) * half_rows)
        here = wb[which, 2 * m : 2 * m + 2].reshape(half_rows, 128)
        norm = row_norm(here.astype(F32), half * DIM)
        tile = jnp.exp2(SCALE * dot(here, rhs[half]) - norm - bias[0:1])
        product = dot(panel[slot, rows], lcol[...])
        for i in range(2):
            sub = slice(i * 128, (i + 1) * 128)
            out_rows = slice(m * half_rows + i * 128, m * half_rows + (i + 1) * 128)
            for j in range(4):
                cols = slice(j * 128, (j + 1) * 128)
                value = tile[sub, cols]
                if j == 2 * m + i:
                    value = value + diagonal
                update_out[0, out_rows, cols] = (value - product[sub, cols]).astype(BF)


def tiles(panel_index, column_map, wb, zc, xp, inverse_factor, panel):
    vmem = pl.BlockSpec(memory_space=pltpu.VMEM)
    hbm = pl.BlockSpec(memory_space=pltpu.HBM)
    flops = 2 * NB * NB * (RW * (128 + NB) + 2 * NB)
    return pl.pallas_call(
        tiles_kernel,
        grid=(RW,),
        out_shape=[
            jax.ShapeDtypeStruct((RW, 16, NB), BF),
            jax.ShapeDtypeStruct((RW, NB, NB), BF),
        ],
        in_specs=[hbm, hbm, vmem, vmem, vmem, vmem, vmem],
        out_specs=[
            pl.BlockSpec((RW, 16, NB), lambda i: (0, 0, 0)),
            pl.BlockSpec((1, NB, NB), lambda i: (i, 0, 0)),
        ],
        scratch_shapes=[
            pltpu.VMEM((2, 128, NB), BF),
            pltpu.VMEM((8, NB), F32),
            pltpu.VMEM((NB, NB), BF),
            pltpu.SMEM((1,), jnp.int32),
            pltpu.SMEM((1,), jnp.int32),
            pltpu.SemaphoreType.DMA((2,)),
        ],
        compiler_params=pltpu.CompilerParams(vmem_limit_bytes=24 << 20),
        cost_estimate=pl.CostEstimate(flops=flops, bytes_accessed=5 << 20, transcendentals=7 * NB * NB),
        name="window_tiles",
    )(panel_index, column_map, wb, zc, xp, inverse_factor, panel)


def shards(points, inverse_factor, panel_index, column_map):
    wb, zc, xp, panel, inv = gathered(panel_index, column_map, points, inverse_factor)
    panel_part, update = tiles(panel_index, column_map, wb, zc, xp, inv, panel)
    return panel_part[:, None], update[:, None, :, None, :]


def solution(mesh):
    in_specs = (P(None, "row", "col", None), P(), P(), P("col"))
    out_specs = (P(None, "row", "col", None), P(None, "row", None, "col", None))
    return jax.shard_map(shards, mesh=mesh, in_specs=in_specs, out_specs=out_specs, check_vma=False)
```

```python
import math

import jax
import jax.numpy as jnp
from jax import lax
from jax.experimental import pallas as pl
from jax.experimental.pallas import tpu as pltpu
from jax.sharding import PartitionSpec as P

RW = 6
JITTER = 1.0
NB = 512
DIM = 64
N_ROW = 16
NX, NZH, NCORE, NZL, NY = 4, 2, 2, 4, 8
NZ = NZH * NZL
NP = NX * NCORE
SCALE = math.log2(math.e) / DIM
MESH = pl.DeviceIdType.MESH
BF = jnp.bfloat16
F32 = jnp.float32


def first_slot(p, r):
    return (p + N_ROW - r) // N_ROW


def assembled(buf):
    low = lax.broadcasted_iota(jnp.int32, (8, 128), 1) < DIM
    parts = []
    for h in range(2):
        packed = buf[h, 0:NZL].astype(F32) + buf[h, NZL:NZ].astype(F32)
        turned = pltpu.roll(packed.reshape(NZL * 4 * 8, 128), DIM, 1).reshape(packed.shape)
        parts.append(jnp.where(low, jnp.concatenate([packed, turned], axis=1), 0.0))
    return jnp.stack(parts, axis=2).reshape(NB, 128)


def packed_pair(a, b, low):
    return jnp.where(low, a, pltpu.roll(b, DIM, 1))


def fill_rhs(block, rhs, bias):
    turned = block.T[0:DIM]
    one = turned.astype(BF)
    none = jnp.zeros_like(one)
    rhs[0] = jnp.concatenate([one, none], axis=0)
    rhs[1] = jnp.concatenate([none, one], axis=0)
    norm = jnp.sum(turned * turned, axis=0, keepdims=True) * (0.5 * SCALE)
    bias[...] = jnp.broadcast_to(norm, (8, NB))


def row_norm(vals, low_lane):
    lanes = lax.broadcasted_iota(jnp.int32, vals.shape, 1)
    inside = (lanes >= low_lane) & (lanes < low_lane + DIM)
    return jnp.sum(jnp.where(inside, vals * vals, 0.0), axis=1, keepdims=True) * (0.5 * SCALE)


def dot(a, b):
    return lax.dot_general(a, b, (((1,), (0,)), ((), ())), preferred_element_type=F32)


def dot_t(a, b):
    return lax.dot_general(a, b, (((1,), (1,)), ((), ())), preferred_element_type=F32)


def gather_kernel(
    p_hbm, cm_hbm, pts_hbm, inv_hbm, wb, zc, xp, panel, inv, mark,
    p_ref, cm_ref, pts_ref, xe, xb, ps, yc, yp, cms, zs, zq, zp, rhs, bias,
    x_s, x_r, c_s, c_r, wy_s, wy_r, wz_s, wz_r, w2y_s, w2y_r, w2z_s, w2z_r,
    yc_s, yc_r, yp_s, yp_r, zp_s, zp_r, zc_s, zc_r, in_s,
):
    row, col = lax.axis_index("row"), lax.axis_index("col")
    x, zh, core = row // 4, (row // 2) % 2, row % 2
    zl, y = col // NY, col % NY
    z = zh * NZL + zl
    q = x * 2 + core

    def dev(x_=x, zh_=zh, core_=core, zl_=zl, y_=y):
        return ((x_ * 2 + zh_) * 2 + core_, zl_ * NY + y_)

    def q_dev(q_):
        return dev(x_=q_ // 2, core_=q_ % 2)

    def z_dev(z_, core_):
        return dev(zh_=z_ // NZL, zl_=z_ % NZL, core_=core_)

    q_peers = [(q + d) % NP for d in range(1, NP)]
    y_peers = [(y + d) % NY for d in (4, 3, 5, 2, 6, 1, 7)]
    z_peers = [(z + d) % NZ for d in (4, 3, 5, 2, 6, 1, 7)]
    l_peers = [(zl + d) % NZL for d in range(1, NZL)]
    line = [(z_, (core + k) % 2) for z_ in z_peers for k in range(2)] + [(z, 1 - core)]

    loads = [
        pltpu.make_async_copy(src, dst, in_s.at[i])
        for i, (src, dst) in enumerate(
            [(p_hbm, p_ref), (cm_hbm, cm_ref), (pts_hbm, pts_ref), (inv_hbm, inv)]
        )
    ]
    for load in loads:
        load.start()

    barrier = pltpu.get_barrier_semaphore()
    greeted = [z_dev(z_, k_) for z_, k_ in line[:-1]] + [dev(y_=y_) for y_ in y_peers] + [q_dev(q_) for q_ in q_peers]
    for to in greeted:
        pl.semaphore_signal(barrier, 1, device_id=to, device_id_type=MESH)

    for load in loads[:3]:
        load.wait()
    p = p_ref[0]

    base = jnp.clip(first_slot(p, row) - 1, 0, pts_ref.shape[0] - RW - 1)
    for t in range(3):
        wb[t, zl, y] = jnp.concatenate([pts_ref[base + 1 + t, 0], pts_ref[base + 4 + t, 0]], axis=1)
    first = pts_ref[base + 1, 0].astype(F32)
    second = pts_ref[base + 2, 0].astype(F32)
    pivot = pts_ref[base, 0].astype(F32)
    cand = jnp.concatenate([first, second], axis=1)
    piv = jnp.concatenate([pivot, jnp.zeros_like(pivot)], axis=1)
    for h in range(2):
        rows = slice(8 * h, 8 * h + 8)
        xe[h, 0] = cand[rows].astype(BF)
        xe[h, 1] = piv[rows].astype(BF)
    xb[q] = xe[core]
    cms[zl] = jnp.full((8, 128), cm_ref[0], jnp.int32).astype(F32)
    mark[...] = jnp.full((8, 128), p + 1 + cm_ref[0] - row - first_slot(p, row) * N_ROW, jnp.int32)
    pl.semaphore_wait(barrier, len(greeted))

    sends = []

    def send(src, dst, ssem, rsem, to):
        copy = pltpu.make_async_remote_copy(
            src_ref=src, dst_ref=dst, send_sem=ssem, recv_sem=rsem, device_id=to, device_id_type=MESH
        )
        copy.start()
        sends.append(copy)

    def arrived(dst, rsem):
        pltpu.make_async_remote_copy(
            src_ref=dst, dst_ref=dst, send_sem=rsem, recv_sem=rsem, device_id=dev(), device_id_type=MESH
        ).wait_recv()

    def send_line(src_of, dst, ssem, rsem):
        for z_, k_ in line:
            send(src_of(z_), dst.at[core, z], ssem.at[k_ * NZ + z_], rsem.at[core * NZ + z], z_dev(z_, k_))

    def line_arrived(dst, rsem):
        for z_, k_ in line:
            arrived(dst.at[k_, z_], rsem.at[k_ * NZ + z_])

    zfirst, yfirst = pl.ds(0, 2), pl.ds(2, 1)
    for q_ in q_peers:
        send(xe.at[q_ % 2], xb.at[q], x_s.at[q_], x_r.at[q], q_dev(q_))
    for l_ in l_peers:
        send(cms.at[zl], cms.at[zl], c_s.at[l_], c_r.at[zl], dev(zl_=l_))
    for y_ in y_peers:
        send(wb.at[yfirst, zl, y], wb.at[yfirst, zl, y], wy_s.at[y_], wy_r.at[y], dev(y_=y_))
    for l_ in l_peers:
        send(wb.at[zfirst, zl, y], wb.at[zfirst, zl, y], wz_s.at[l_], wz_r.at[zl], dev(zl_=l_))

    for q_ in q_peers:
        arrived(xb.at[q_], x_r.at[q_])
    mine = jnp.zeros((8, 128), F32)
    for k in range(NP):
        r = ((k // 2) * 2 + zh) * 2 + k % 2
        mine += jnp.where(r == p % N_ROW, xb[k, 1].astype(F32), 0.0)
    ps[...] = mine.astype(BF)
    yp[y] = mine.astype(BF)
    yc[y] = xb[:, 0]
    for y_ in y_peers:
        send(ps, yp.at[y], yp_s.at[y_], yp_r.at[y], dev(y_=y_))
    for y_ in y_peers:
        send(xb.at[:, 0], yc.at[y], yc_s.at[y_], yc_r.at[y], dev(y_=y_))

    for l_ in l_peers:
        arrived(wb.at[zfirst, l_, y], wz_r.at[l_])
    for y_ in y_peers:
        send(wb.at[zfirst, :, y], wb.at[zfirst, :, y], w2y_s.at[y_], w2y_r.at[y], dev(y_=y_))
    for y_ in y_peers:
        arrived(wb.at[yfirst, zl, y_], wy_r.at[y_])
    for l_ in l_peers:
        send(wb.at[yfirst, zl], wb.at[yfirst, zl], w2z_s.at[l_], w2z_r.at[zl], dev(zl_=l_))

    low = lax.broadcasted_iota(jnp.int32, (8, 128), 1) < DIM
    for y_ in y_peers:
        arrived(yp.at[y_], yp_r.at[y_])
    for k in range(4):
        zq[k] = packed_pair(yp[k].astype(F32), yp[k + 4].astype(F32), low).astype(BF)
    zp[core, z] = zq[...]
    early = len(sends)
    send_line(lambda z_: zq, zp, zp_s, zp_r)

    for l_ in l_peers:
        arrived(cms.at[l_], c_r.at[l_])
    wanted = [cms[l_] for l_ in range(NZL)]
    ranks = []
    for k in range(NP):
        r = ((k // 2) * 2 + zh) * 2 + k % 2
        own = first_slot(p, r) * N_ROW + r - p - 1
        ranks.append(jnp.where(low, own, own + N_ROW).astype(F32))
    for y_ in y_peers:
        arrived(yc.at[y_], yc_r.at[y_])
    for k4 in range(4):
        chosen = [[], []]
        for i in range(2):
            tiles = [yc[k4 + 4 * i, k].astype(F32) for k in range(NP)]
            for l_ in range(NZL):
                total = jnp.zeros((8, 128), F32)
                for k in range(NP):
                    total = jnp.where(wanted[l_] == ranks[k], tiles[k], total)
                chosen[i].append(total + pltpu.roll(total, DIM, 1))
        for l_ in range(NZL):
            zs[l_, k4] = jnp.where(low, chosen[0][l_], chosen[1][l_]).astype(BF)
    zc[core, z] = zs[zl]
    send_line(lambda z_: zs.at[z_ % NZL], zc, zc_s, zc_r)

    for copy in sends[:early]:
        copy.wait_send()
    line_arrived(zp, zp_r)
    pivots = assembled(zp)
    xp[...] = pivots.astype(BF)
    fill_rhs(pivots, rhs, bias)
    for l_ in l_peers:
        arrived(wb.at[yfirst, l_], w2z_r.at[l_])
    for y_ in y_peers:
        arrived(wb.at[zfirst, :, y_], w2y_r.at[y_])

    loads[3].wait()
    half_rows = NB // 2

    @pl.loop(0, RW)
    def _(slot):
        which, half = slot % 3, slot // 3
        for m in range(2):
            rows = slice(m * half_rows, (m + 1) * half_rows)
            here = wb[which, 2 * m : 2 * m + 2].reshape(half_rows, 128)
            norm = row_norm(here.astype(F32), half * DIM)
            kpanel = jnp.exp2(SCALE * dot(here, rhs[half]) - norm - bias[0:1]).astype(BF)
            panel[slot, rows, 0:half_rows] = dot_t(
                kpanel[:, 0:half_rows], inv[0:half_rows, 0:half_rows]
            ).astype(BF)
            panel[slot, rows, half_rows:NB] = dot_t(kpanel, inv[half_rows:NB]).astype(BF)

    line_arrived(zc, zc_r)
    for copy in sends[early:]:
        copy.wait_send()


def gathered(panel_index, column_map, points, inverse_factor):
    vmem = pl.BlockSpec(memory_space=pltpu.VMEM)
    hbm = pl.BlockSpec(memory_space=pltpu.HBM)
    dma = pltpu.SemaphoreType.DMA
    counts = [NP, NP, NZL, NZL, NY, NY, NZL, NZL, NY, NY, NZL, NZL, NY, NY, NY, NY] + [2 * NZ] * 4 + [4]
    return pl.pallas_call(
        gather_kernel,
        out_shape=[
            pltpu.VMEM((3, NZL, NY, 16, 128), BF),
            pltpu.VMEM((2, NZ, 4, 8, 128), BF),
            pltpu.VMEM((NB, 128), BF),
            pltpu.VMEM((RW, NB, NB), BF),
            pltpu.VMEM((NB, NB), BF),
            pltpu.VMEM((8, 128), jnp.int32),
        ],
        in_specs=[hbm] * 4,
        out_specs=[vmem] * 6,
        scratch_shapes=[
            pltpu.SMEM((1,), jnp.int32),
            pltpu.SMEM((1,), jnp.int32),
            pltpu.VMEM(points.shape, BF),
            pltpu.VMEM((2, 2, 8, 128), BF),
            pltpu.VMEM((NP, 2, 8, 128), BF),
            pltpu.VMEM((8, 128), BF),
            pltpu.VMEM((NY, NP, 8, 128), BF),
            pltpu.VMEM((NY, 8, 128), BF),
            pltpu.VMEM((NZL, 8, 128), F32),
            pltpu.VMEM((NZL, 4, 8, 128), BF),
            pltpu.VMEM((4, 8, 128), BF),
            pltpu.VMEM((2, NZ, 4, 8, 128), BF),
            pltpu.VMEM((2, 128, NB), BF),
            pltpu.VMEM((8, NB), F32),
        ]
        + [dma((n,)) for n in counts],
        compiler_params=pltpu.CompilerParams(collective_id=0, has_side_effects=True, vmem_limit_bytes=61100 << 10),
        name="gather_panel",
    )(panel_index, column_map, points, inverse_factor)


def tiles_kernel(mark, wb, zc, xp, inv, panel, panel_out, update_out, rhs, bias, lcol):
    slot = pl.program_id(0)
    col = lax.axis_index("col")
    half_rows = NB // 2

    @pl.when(slot == 0)
    def _():
        fill_rhs(assembled(zc), rhs, bias)
        norm = row_norm(xp[...].astype(F32), 0)
        cross = jnp.exp2(SCALE * dot(xp[...], rhs[0]) - norm - bias[0:1]).astype(BF)
        lcol[0:half_rows] = dot(inv[0:half_rows, 0:half_rows], cross[0:half_rows]).astype(BF)
        lcol[half_rows:NB] = dot(inv[half_rows:NB], cross).astype(BF)
        start = pl.multiple_of(col * 16, 16)
        for a in range(RW):
            panel_out[a] = panel[a, pl.ds(start, 16)]
    which, half = slot % 3, slot // 3
    here_too = mark[0:1] == slot * N_ROW
    eye = lax.broadcasted_iota(jnp.int32, (128, 128), 0) == lax.broadcasted_iota(jnp.int32, (128, 128), 1)
    diagonal = jnp.where(eye & here_too, JITTER, 0.0)
    here = wb[which].reshape(NB, 128)
    norm = row_norm(here.astype(F32), half * DIM)
    for n in range(2):
        side = slice(n * half_rows, (n + 1) * half_rows)
        tile = jnp.exp2(SCALE * dot(here, rhs[half, :, side]) - norm - bias[0:1, side])
        product = dot(panel[slot], lcol[:, side])
        for i in range(4):
            sub = slice(i * 128, (i + 1) * 128)
            for j in range(2):
                cols = slice(j * 128, (j + 1) * 128)
                value = tile[sub, cols]
                if 2 * n + j == i:
                    value = value + diagonal
                out_cols = slice(n * half_rows + j * 128, n * half_rows + (j + 1) * 128)
                update_out[0, sub, out_cols] = (value - product[sub, cols]).astype(BF)


def tiles(mark, wb, zc, xp, inverse_factor, panel):
    vmem = pl.BlockSpec(memory_space=pltpu.VMEM)
    flops = 2 * NB * NB * (RW * (128 + NB) + 2 * NB)
    return pl.pallas_call(
        tiles_kernel,
        grid=(RW,),
        out_shape=[
            jax.ShapeDtypeStruct((RW, 16, NB), BF),
            jax.ShapeDtypeStruct((RW, NB, NB), BF),
        ],
        in_specs=[vmem] * 6,
        out_specs=[
            pl.BlockSpec((RW, 16, NB), lambda i: (0, 0, 0)),
            pl.BlockSpec((1, NB, NB), lambda i: (i, 0, 0)),
        ],
        scratch_shapes=[
            pltpu.VMEM((2, 128, NB), BF),
            pltpu.VMEM((8, NB), F32),
            pltpu.VMEM((NB, NB), BF),
        ],
        compiler_params=pltpu.CompilerParams(vmem_limit_bytes=24 << 20),
        cost_estimate=pl.CostEstimate(flops=flops, bytes_accessed=5 << 20, transcendentals=7 * NB * NB),
        name="window_tiles",
    )(mark, wb, zc, xp, inverse_factor, panel)


def shards(points, inverse_factor, panel_index, column_map):
    wb, zc, xp, panel, inv, mark = gathered(panel_index, column_map, points, inverse_factor)
    panel_part, update = tiles(mark, wb, zc, xp, inv, panel)
    return panel_part[:, None], update[:, None, :, None, :]


def solution(mesh):
    in_specs = (P(None, "row", "col", None), P(), P(), P("col"))
    out_specs = (P(None, "row", "col", None), P(None, "row", None, "col", None))
    return jax.shard_map(shards, mesh=mesh, in_specs=in_specs, out_specs=out_specs, check_vma=False)
```
